32 devices in a mesh: problem: 1 (over z), samp: 4 (over y), feat: 8 (over x, core).
Axes of the slice: x: 4, y: 4, z: 1, core: 2. Of those that a mesh axis runs over, the one named last changes fastest.
The devices are a block of a 4x4x8 slice.
Arguments:
- design: bfloat16 [16384, 32768], P(('problem', 'samp'), 'feat')
- targets: float32 [16384, 128], P(('problem', 'samp'))
- coef_init: float32 [32768, 128], P(('problem', 'feat'))
- step_sizes: float32 [32768], P(('problem', 'feat'))
- ridge_weights: float32 [128], P('problem')
Outputs:
- output 1: float32 [32768, 128], P(('problem', 'feat'))
- output 2: float32 [16384, 128], P(('problem', 'samp'))
All inputs are finite; a program needn't handle non-finite values.
Results may differ from the reference program's by a relative error of at most 0.00671238.
Values are sent between devices in bfloat16 or wider.
A program may use at most 768 MiB of HBM per device.

```python
import jax
import jax.numpy as jnp
from jax import lax

NUM_ROWS = 16384
NUM_FEATURES = 32768
NUM_TARGETS = 128
FEAT_BLOCKS = 8
SWEEPS = 4
STEP_WEIGHT = 0.5


def setup_inputs(seed: int = 0, part: int = 0) -> dict:
    base_key = jax.random.fold_in(jax.random.key(seed), part)
    sub_keys = jax.random.split(base_key, 9)
    shared_rank = 8
    shared_mix = 0.8
    row_block = NUM_ROWS // 8
    factors = jax.random.normal(sub_keys[0], (NUM_ROWS, shared_rank), jnp.float32)
    loadings = jax.random.normal(sub_keys[1], (shared_rank, NUM_FEATURES), jnp.float32)

    def draw_rows(block_index):
        rows_f = lax.dynamic_slice_in_dim(factors, block_index * row_block, row_block, 0)
        shared = jnp.dot(rows_f, loadings) * (shared_mix / shared_rank) ** 0.5
        noise_blk = jax.random.normal(jax.random.fold_in(sub_keys[2], block_index), (row_block, NUM_FEATURES), jnp.float32)
        return (shared + (1.0 - shared_mix) ** 0.5 * noise_blk).astype(jnp.bfloat16)

    design = lax.map(draw_rows, jnp.arange(8)).reshape(NUM_ROWS, NUM_FEATURES)

    def power_step(step_index, probe_vec):
        unit_vec = probe_vec / jnp.linalg.norm(probe_vec)
        image_vec = jnp.dot(design, unit_vec.astype(jnp.bfloat16), preferred_element_type=jnp.float32)
        return jnp.dot(image_vec.astype(jnp.bfloat16), design, preferred_element_type=jnp.float32) / NUM_ROWS

    probe_init = jax.random.normal(sub_keys[3], (NUM_FEATURES,), jnp.float32)
    curvature = 1.15 * jnp.linalg.norm(lax.fori_loop(0, 12, power_step, probe_init))
    step_sizes = jax.random.uniform(sub_keys[4], (NUM_FEATURES,), jnp.float32, 0.4, 0.8) / curvature
    ridge_weights = jax.random.uniform(sub_keys[5], (NUM_TARGETS,), jnp.float32, 0.05, 0.25) * curvature
    coef_init = jax.random.normal(sub_keys[6], (NUM_FEATURES, NUM_TARGETS), jnp.float32) * NUM_FEATURES ** -0.5
    w_star = jax.random.normal(sub_keys[7], (NUM_FEATURES, NUM_TARGETS), jnp.float32) * NUM_FEATURES ** -0.5
    targets = jnp.dot(design, w_star.astype(jnp.bfloat16), preferred_element_type=jnp.float32) + 0.3 * jax.random.normal(sub_keys[8], (NUM_ROWS, NUM_TARGETS), jnp.float32)
    return {"design": design, "targets": targets, "coef_init": coef_init, "step_sizes": step_sizes, "ridge_weights": ridge_weights}


def reference(design, targets, coef_init, step_sizes, ridge_weights):
    block_cols = NUM_FEATURES // FEAT_BLOCKS

    def block_sum(weights):
        weights_b = weights.astype(jnp.bfloat16)

        def add_block(acc_sum, block_index):
            col_block = lax.dynamic_slice_in_dim(design, block_index * block_cols, block_cols, 1)
            rows_w = lax.dynamic_slice_in_dim(weights_b, block_index * block_cols, block_cols, 0)
            product = jnp.dot(col_block, rows_w, preferred_element_type=jnp.float32)
            return acc_sum + product.astype(jnp.bfloat16).astype(jnp.float32), None

        return lax.scan(add_block, jnp.zeros((NUM_ROWS, NUM_TARGETS), jnp.float32), jnp.arange(FEAT_BLOCKS))[0]

    def sweep_once(sweep_state, unused):
        coef_cur, resid_cur = sweep_state
        gradient = lax.dot_general(design, resid_cur.astype(jnp.bfloat16), (((0,), (0,)), ((), ())), preferred_element_type=jnp.float32) / NUM_ROWS
        step_delta = step_sizes[:, None] * (gradient - ridge_weights[None, :] * coef_cur)
        return (coef_cur + STEP_WEIGHT * step_delta, resid_cur - STEP_WEIGHT * block_sum(step_delta)), None

    start_state = (coef_init, targets - block_sum(coef_init))
    final_state = lax.scan(sweep_once, start_state, None, length=SWEEPS)[0]
    return final_state[0], final_state[1]
```

```python
import functools

import jax
import jax.numpy as jnp
from jax import lax
from jax.experimental import pallas as pl
from jax.experimental.pallas import tpu as pltpu
from jax.sharding import PartitionSpec as P

SWEEPS = 4
STEP_WEIGHT = 0.5
CORES = 2
NT = (((1,), (1,)), ((), ()))
MESH = pl.DeviceIdType.MESH
BF16 = jnp.bfloat16
F32 = jnp.float32


def sweeps_kernel(ny, nf, x_hbm, y_hbm, w0_hbm, eta_ref, lam_ref, w_out, r_out,
                  x, st, rt, gp, yb, ub, sb, pb, xb, wt, res,
                  xsem, lsem, sib_s, sib_r, xs_s, xs_r, ys_s, ys_r,
                  xg_s, xg_r, xp_s, xp_r, yg_s, yg_r, wg_s, wg_r, rg_s, rg_r, rp_s, rp_r):
    nx = nf // CORES
    rows, feats = x.shape
    targets = wt.shape[0]
    rc = rows // nf
    rh = rc // 2
    fc = feats // ny
    fh = fc // 2
    inv_total = 1.0 / (rows * ny)

    yi = lax.axis_index("samp")
    fi = lax.axis_index("feat")
    chip = fi // CORES
    core = fi % CORES
    y_up, y_dn = (yi + 1) % ny, (yi + ny - 1) % ny
    y_op = (yi + 2) % ny
    c_up, c_dn = (chip + 1) % nx, (chip + nx - 1) % nx
    c_op = (chip + 2) % nx
    UP = {"feat": c_up * CORES + core}
    DN = {"feat": c_dn * CORES + core}
    SIB = {"feat": chip * CORES + 1 - core}
    YUP = {"samp": y_up}
    YDN = {"samp": y_dn}

    def rcopy(src, dst, ss, rs, dev):
        return pltpu.make_async_remote_copy(src_ref=src, dst_ref=dst, send_sem=ss, recv_sem=rs,
                                            device_id=dev, device_id_type=MESH)

    def lanes(start, size):
        return pl.ds(pl.multiple_of(start, 128), size)

    def srows(start, size):
        return pl.ds(pl.multiple_of(start, 128), size)

    def ring_off(j):
        return (2 + 3 * j + 3 * (j // 2) + 2 * (j // 3)) % 4

    def row_chunk(i):
        j, who = i // 2, i % 2
        d = (chip + ring_off(j)) % nx
        return d * CORES + core + (1 - who) * (1 - 2 * core)

    def xload(i):
        c = row_chunk(i)
        return pltpu.make_async_copy(x_hbm.at[srows(c * rc, rc), :], x.at[srows(c * rc, rc), :], xsem.at[i])

    w0_copy = pltpu.make_async_copy(w0_hbm, w_out, lsem.at[0])
    y_copy = pltpu.make_async_copy(y_hbm.at[srows(fi * rc, rc), :], res, lsem.at[1])
    w0_copy.start()
    for i in range(nf):
        xload(i).start()
    y_copy.start()

    barrier = pltpu.get_barrier_semaphore()
    peers = (UP, DN, SIB, YUP, YDN)
    for dev in peers:
        pl.semaphore_signal(barrier, inc=1, device_id=dev, device_id_type=MESH)

    w0_copy.wait()

    def w0_step(i, c):
        blk = w_out[srows(i * rc, rc), :]
        st[:, lanes(i * rc, rc)] = jnp.transpose(blk).astype(BF16)
        return c
    lax.fori_loop(0, feats // rc, w0_step, 0)
    for h in range(2):
        wt[:, pl.ds(h * fh, fh)] = jnp.transpose(w_out[srows(yi * fc + h * fh, fh), :])
    pl.semaphore_wait(barrier, len(peers))
    y_copy.wait()

    def sib_copy(j):
        return rcopy(ub.at[2 * j], sb.at[j], sib_s.at[j], sib_r.at[j], SIB)

    H0, H1 = pl.ds(0, rh), pl.ds(rh, rh)
    x_rs = [
        lambda: rcopy(pb.at[0, H0], xb.at[0], xs_s.at[0], xs_r.at[0], UP),
        lambda: rcopy(pb.at[0, H1], xb.at[1], xs_s.at[1], xs_r.at[1], DN),
        lambda: rcopy(pb.at[1, H1], xb.at[2], xs_s.at[2], xs_r.at[2], UP),
        lambda: rcopy(pb.at[2, H0], xb.at[3], xs_s.at[3], xs_r.at[3], DN),
        lambda: rcopy(pb.at[1, H0], xb.at[4], xs_s.at[4], xs_r.at[4], UP),
        lambda: rcopy(pb.at[2, H1], xb.at[5], xs_s.at[5], xs_r.at[5], DN),
    ]

    def gsl(d, h):
        return gp.at[:, lanes(d * fc + h * fh, fh)]
    y_rs = [
        lambda: rcopy(gsl(y_op, 0), yb.at[0], ys_s.at[0], ys_r.at[0], YUP),
        lambda: rcopy(gsl(y_op, 1), yb.at[1], ys_s.at[1], ys_r.at[1], YDN),
        lambda: rcopy(gsl(y_up, 1), yb.at[2], ys_s.at[2], ys_r.at[2], YUP),
        lambda: rcopy(gsl(y_dn, 0), yb.at[3], ys_s.at[3], ys_r.at[3], YDN),
        lambda: rcopy(gsl(y_up, 0), yb.at[4], ys_s.at[4], ys_r.at[4], YUP),
        lambda: rcopy(gsl(y_dn, 1), yb.at[5], ys_s.at[5], ys_r.at[5], YDN),
    ]

    def gather(piece, ss, rs, up, dn, me, below, above):
        return [
            lambda: rcopy(piece(me, 0), piece(me, 0), ss.at[0], rs.at[0], up),
            lambda: rcopy(piece(me, 1), piece(me, 1), ss.at[1], rs.at[1], up),
            lambda: rcopy(piece(me, 0), piece(me, 0), ss.at[2], rs.at[2], dn),
            lambda: rcopy(piece(me, 1), piece(me, 1), ss.at[3], rs.at[3], dn),
            lambda: rcopy(piece(below, 0), piece(below, 0), ss.at[4], rs.at[4], up),
            lambda: rcopy(piece(above, 1), piece(above, 1), ss.at[5], rs.at[5], dn),
        ]

    y_ag = gather(lambda d, h: st.at[:, lanes(d * fc + h * fh, fh)], yg_s, yg_r, YUP, YDN, yi, y_dn, y_up)
    x_ag = gather(lambda d, h: rt.at[:, lanes((d * CORES + core) * rc + h * rh, rh)], xg_s, xg_r, UP, DN, chip, c_dn, c_up)
    w_ag = gather(lambda d, h: w_out.at[srows(d * fc + h * fh, fh), :], wg_s, wg_r, YUP, YDN, yi, y_dn, y_up)
    r_ag = gather(lambda d, h: r_out.at[srows((d * CORES + core) * rc + h * rh, rh), :], rg_s, rg_r, UP, DN, chip, c_dn, c_up)

    def pair(piece, half, ss, rs):
        return [
            lambda: rcopy(piece(chip), piece(chip), ss.at[0], rs.at[0], SIB),
            lambda: rcopy(piece(c_dn), piece(c_dn), ss.at[1], rs.at[1], SIB),
            lambda: rcopy(piece(c_up), piece(c_up), ss.at[2], rs.at[2], SIB),
            lambda: rcopy(half(c_op, 0), half(c_op, 0), ss.at[3], rs.at[3], SIB),
            lambda: rcopy(half(c_op, 1), half(c_op, 1), ss.at[4], rs.at[4], SIB),
        ]
    x_pair = pair(lambda d: rt.at[:, lanes((d * CORES + core) * rc, rc)],
                  lambda d, h: rt.at[:, lanes((d * CORES + core) * rc + h * rh, rh)], xp_s, xp_r)
    r_pair = pair(lambda d: r_out.at[srows((d * CORES + core) * rc, rc), :],
                  lambda d, h: r_out.at[srows((d * CORES + core) * rc + h * rh, rh), :], rp_s, rp_r)

    def ring_and_pair(ag, pr):
        ag[0]().wait_recv()
        ag[4]().start()
        ag[3]().wait_recv()
        ag[5]().start()
        ag[1]().wait_recv()
        pr[1]().start()
        ag[2]().wait_recv()
        pr[2]().start()
        ag[4]().wait_recv()
        pr[3]().start()
        ag[5]().wait_recv()
        pr[4]().start()
        for c in pr:
            c().wait_recv()

    def sweep(k, carry):
        def u_step(i, c):
            j, who = i // 2, i % 2

            @pl.when(k == 0)
            def _():
                xload(i).wait()
            u = lax.dot_general(x[srows(row_chunk(i) * rc, rc), :], st[...], NT, preferred_element_type=F32)
            ub[i] = u.astype(BF16)

            @pl.when(who == 0)
            def _():
                sib_copy(j).start()

            @pl.when(who == 1)
            def _():
                sib_copy(j).wait_recv()
                pb[j] = ub[i].astype(F32) + sb[j].astype(F32)

            @pl.when(i == 1)
            def _():
                x_rs[0]().start()
                x_rs[1]().start()

            @pl.when(i == 3)
            def _():
                x_rs[2]().start()

            @pl.when(i == 5)
            def _():
                x_rs[3]().start()
                x_rs[0]().wait_recv()
                pb[1, H0] = pb[1, H0] + xb[0]
                x_rs[4]().start()
                x_rs[1]().wait_recv()
                pb[2, H1] = pb[2, H1] + xb[1]
                x_rs[5]().start()
            return c
        lax.fori_loop(0, nf, u_step, 0)

        scale = jnp.where(k == 0, 1.0, STEP_WEIGHT).astype(F32)
        x_rs[3]().wait_recv()
        x_rs[4]().wait_recv()
        res[H0] = res[H0] - scale * (pb[3, H0] + xb[3] + xb[4])
        x_rs[2]().wait_recv()
        x_rs[5]().wait_recv()
        res[H1] = res[H1] - scale * (pb[3, H1] + xb[2] + xb[5])

        @pl.when(k < SWEEPS)
        def _():
            rt[:, lanes(fi * rc, rh)] = jnp.transpose(res[H0]).astype(BF16)
            x_ag[0]().start()
            x_ag[2]().start()
            rt[:, lanes(fi * rc + rh, rh)] = jnp.transpose(res[H1]).astype(BF16)
            x_ag[3]().start()
            x_ag[1]().start()
            x_pair[0]().start()
            for j in range(nx):
                sib_copy(j).wait_send()
            for c in x_rs:
                c().wait_send()
            ring_and_pair(x_ag, x_pair)

            def g_step(i, c):
                j, h = i // 2, i % 2
                col = lanes(((yi + ring_off(j)) % ny) * fc + h * fh, fh)
                gp[:, col] = jnp.dot(rt[...], x[:, col], preferred_element_type=F32)
                for step, n in ((0, 0), (1, 1), (3, 2), (4, 3)):
                    @pl.when(i == step)
                    def _():
                        y_rs[n]().start()
                return c
            lax.fori_loop(0, 2 * ny, g_step, 0)
            for c in x_ag + x_pair:
                c().wait_send()
            y_rs[0]().wait_recv()
            up0 = lanes(y_up * fc, fh)
            gp[:, up0] = gp[:, up0] + yb[0]
            y_rs[4]().start()
            y_rs[1]().wait_recv()
            dn1 = lanes(y_dn * fc + fh, fh)
            gp[:, dn1] = gp[:, dn1] + yb[1]
            y_rs[5]().start()

            def s_half(h, a, b):
                own = lanes(yi * fc + h * fh, fh)
                wsl = pl.ds(h * fh, fh)
                g = (gp[:, own] + yb[a] + yb[b]) * inv_total
                w = wt[:, wsl]
                s = eta_ref[:, own] * (g - lam_ref[...] * w)
                wt[:, wsl] = w + STEP_WEIGHT * s
                st[:, own] = s.astype(BF16)

            y_rs[3]().wait_recv()
            y_rs[4]().wait_recv()
            s_half(0, 3, 4)
            y_ag[0]().start()
            y_rs[2]().wait_recv()
            y_rs[5]().wait_recv()
            s_half(1, 2, 5)
            y_ag[3]().start()
            y_ag[1]().start()
            y_ag[2]().start()
            for c in y_rs:
                c().wait_send()

            @pl.when(k == SWEEPS - 1)
            def _():
                for h in range(2):
                    w_out[srows(yi * fc + h * fh, fh), :] = jnp.transpose(wt[:, pl.ds(h * fh, fh)])
            y_ag[0]().wait_recv()
            y_ag[4]().start()
            y_ag[3]().wait_recv()
            y_ag[5]().start()
            for n in (1, 2, 4, 5):
                y_ag[n]().wait_recv()

            @pl.when(k == SWEEPS - 1)
            def _():
                for n in (0, 3, 1, 2):
                    w_ag[n]().start()
            for c in y_ag:
                c().wait_send()
        return carry

    lax.fori_loop(0, SWEEPS + 1, sweep, 0)

    r_out[srows(fi * rc, rc), :] = res[...]
    for n in (0, 3, 1, 2):
        r_ag[n]().start()
    r_pair[0]().start()
    w_ag[0]().wait_recv()
    w_ag[4]().start()
    w_ag[3]().wait_recv()
    w_ag[5]().start()
    for j in range(nx):
        sib_copy(j).wait_send()
    for c in x_rs:
        c().wait_send()
    ring_and_pair(r_ag, r_pair)
    for n in (1, 2, 4, 5):
        w_ag[n]().wait_recv()
    for c in w_ag + r_ag + r_pair:
        c().wait_send()


def solution(mesh):
    ny, nf = mesh.shape["samp"], mesh.shape["feat"]
    design_spec = P(("problem", "samp"), "feat")
    rows_spec = P(("problem", "samp"), None)
    coef_spec = P(("problem", "feat"), None)
    step_spec = P(("problem", "feat"))
    ridge_spec = P("problem")

    def local_sweeps(design, targets, coef_init, step_sizes, ridge_weights):
        rows, feats = design.shape
        nt = targets.shape[1]
        rc, fc = rows // nf, feats // ny
        nx = nf // CORES
        dma = lambda n: pltpu.SemaphoreType.DMA((n,))
        anyspec = pl.BlockSpec(memory_space=pl.ANY)
        vspec = pl.BlockSpec(memory_space=pltpu.VMEM)
        return pl.pallas_call(
            functools.partial(sweeps_kernel, ny, nf),
            out_shape=(jax.ShapeDtypeStruct((feats, nt), F32), jax.ShapeDtypeStruct((rows, nt), F32)),
            in_specs=[anyspec, anyspec, anyspec, vspec, vspec],
            out_specs=(vspec, vspec),
            scratch_shapes=[
                pltpu.VMEM((rows, feats), BF16),
                pltpu.VMEM((nt, feats), BF16),
                pltpu.VMEM((nt, rows), BF16),
                pltpu.VMEM((nt, feats), F32),
                pltpu.VMEM((6, nt, fc // 2), F32),
                pltpu.VMEM((nf, rc, nt), BF16),
                pltpu.VMEM((nx, rc, nt), BF16),
                pltpu.VMEM((nx, rc, nt), F32),
                pltpu.VMEM((6, rc // 2, nt), F32),
                pltpu.VMEM((nt, fc), F32),
                pltpu.VMEM((rc, nt), F32),
                dma(nf), dma(2), dma(nx), dma(nx), dma(6), dma(6), dma(6), dma(6),
                dma(6), dma(6), dma(5), dma(5), dma(6), dma(6), dma(6), dma(6), dma(6), dma(6), dma(5), dma(5),
            ],
            compiler_params=pltpu.CompilerParams(
                collective_id=0, has_side_effects=True, vmem_limit_bytes=60 * 1024 * 1024),
            name="sweeps",
        )(design, targets, coef_init, step_sizes[None, :], ridge_weights[:, None])

    return jax.shard_map(local_sweeps, mesh=mesh, in_specs=(design_spec, rows_spec, coef_spec, step_spec, ridge_spec),
                         out_specs=(coef_spec, rows_spec), check_vma=False)
```

```python
import functools

import jax
import jax.numpy as jnp
from jax import lax
from jax.experimental import pallas as pl
from jax.experimental.pallas import tpu as pltpu
from jax.sharding import PartitionSpec as P

SWEEPS = 4
STEP_WEIGHT = 0.5
CORES = 2
NT = (((1,), (1,)), ((), ()))
MESH = pl.DeviceIdType.MESH
BF16 = jnp.bfloat16
F32 = jnp.float32


def sweeps_kernel(ny, nf, x_hbm, y_hbm, w0_hbm, eta_ref, lam_ref, w_out, r_out,
                  x, st, rt, gp, yb, ub, sb, pb, xb, wt, res, ua, w0b, lam_col,
                  xsem, lsem, sib_s, sib_r, xs_s, xs_r, ys_s, ys_r,
                  xg_s, xg_r, xp_s, xp_r, yg_s, yg_r, wg_s, wg_r, rg_s, rg_r, rp_s, rp_r):
    nx = nf // CORES
    rows, feats = x.shape
    targets = wt.shape[0]
    rc = rows // nf
    rh = rc // 2
    fc = feats // ny
    fh = fc // 2
    inv_total = 1.0 / (rows * ny)

    yi = lax.axis_index("samp")
    fi = lax.axis_index("feat")
    chip = fi // CORES
    core = fi % CORES
    y_up, y_dn = (yi + 1) % ny, (yi + ny - 1) % ny
    y_op = (yi + 2) % ny
    c_up, c_dn = (chip + 1) % nx, (chip + nx - 1) % nx
    c_op = (chip + 2) % nx
    UP = {"feat": c_up * CORES + core}
    DN = {"feat": c_dn * CORES + core}
    SIB = {"feat": chip * CORES + 1 - core}
    YUP = {"samp": y_up}
    YDN = {"samp": y_dn}

    def rcopy(src, dst, ss, rs, dev):
        return pltpu.make_async_remote_copy(src_ref=src, dst_ref=dst, send_sem=ss, recv_sem=rs,
                                            device_id=dev, device_id_type=MESH)

    def lanes(start, size):
        return pl.ds(pl.multiple_of(start, 128), size)

    def srows(start, size):
        return pl.ds(pl.multiple_of(start, 128), size)

    def ring_off(j):
        return (2 + 3 * j + 3 * (j // 2) + 2 * (j // 3)) % 4

    def row_chunk(i):
        j, who = i // 2, i % 2
        d = (chip + ring_off(j)) % nx
        return d * CORES + core + (1 - who) * (1 - 2 * core)

    def xload(i):
        c = row_chunk(i)
        return pltpu.make_async_copy(x_hbm.at[srows(c * rc, rc), :], x.at[srows(c * rc, rc), :], xsem.at[i])

    w0_copy = pltpu.make_async_copy(w0_hbm, w_out, lsem.at[0])
    y_copy = pltpu.make_async_copy(y_hbm.at[srows(fi * rc, rc), :], res, lsem.at[1])
    w0_copy.start()
    for i in range(1):
        xload(i).start()
    y_copy.start()

    barrier = pltpu.get_barrier_semaphore()
    peers = (UP, DN, SIB, YUP, YDN)
    for dev in peers:
        pl.semaphore_signal(barrier, inc=1, device_id=dev, device_id_type=MESH)

    w0_copy.wait()
    for i in range(1, 3):
        xload(i).start()

    w0b[...] = w_out[...].astype(BF16)
    lam_col[...] = jnp.transpose(jnp.broadcast_to(lam_ref[...], (lam_col.shape[1], targets)))
    for h in range(2):
        wt[:, pl.ds(h * fh, fh)] = jnp.transpose(w_out[srows(yi * fc + h * fh, fh), :])
    pl.semaphore_wait(barrier, len(peers))
    y_copy.wait()

    PIECES = range(2)
    rq, fq = rc // 4, fc // 4

    def wait_sends(copies):
        for c in copies:
            c.wait_send()

    def sib_copy(j):
        return rcopy(ub.at[2 * j], sb.at[j], sib_s.at[j], sib_r.at[j], SIB)

    def rpos(p, h):
        return pl.ds(p * rh + h * rq, rq)

    def x_rs(p, n):
        j, h = ((0, 0), (0, 1), (1, 1), (2, 0), (1, 0), (2, 1))[n]
        return rcopy(pb.at[j, rpos(p, h)], xb.at[6 * p + n], xs_s.at[6 * p + n], xs_r.at[6 * p + n], (UP, DN)[n % 2])

    def gpos(d, p, h):
        return lanes(d * fc + p * fh + h * fq, fq)

    def y_rs(p, n):
        d, h = ((y_op, 0), (y_op, 1), (y_up, 1), (y_dn, 0), (y_up, 0), (y_dn, 1))[n]
        return rcopy(gp.at[:, gpos(d, p, h)], yb.at[6 * p + n], ys_s.at[6 * p + n], ys_r.at[6 * p + n], (YUP, YDN)[n % 2])

    def ring(at, ss, rs, up, dn, me, below, above):
        def copy(p, n):
            d, h = ((me, 0), (me, 1), (me, 1), (me, 0), (below, 0), (above, 1))[n]
            src = at(d, p, h)
            return rcopy(src, src, ss.at[6 * p + n], rs.at[6 * p + n], (up, dn)[n % 2])
        return copy

    def xpos(d, p, h):
        return (d * CORES + core) * rc + p * rh + h * rq

    def wpos(d, p, h):
        return srows(d * fc + p * fh + h * fq, fq)

    y_ag = ring(lambda d, p, h: st.at[:, gpos(d, p, h)], yg_s, yg_r, YUP, YDN, yi, y_dn, y_up)
    x_ag = ring(lambda d, p, h: rt.at[:, lanes(xpos(d, p, h), rq)], xg_s, xg_r, UP, DN, chip, c_dn, c_up)
    w_ag = ring(lambda d, p, h: w_out.at[wpos(d, p, h), :], wg_s, wg_r, YUP, YDN, yi, y_dn, y_up)
    r_ag = ring(lambda d, p, h: r_out.at[srows(xpos(d, p, h), rq), :], rg_s, rg_r, UP, DN, chip, c_dn, c_up)

    def pair(at, ss, rs):
        def copy(p, n):
            d, h, size = ((chip, 0, rh), (c_dn, 0, rh), (c_up, 0, rh), (c_op, 0, rq), (c_op, 1, rq))[n]
            src = at(xpos(d, p, h), size)
            return rcopy(src, src, ss.at[5 * p + n], rs.at[5 * p + n], SIB)
        return copy

    x_pair = pair(lambda o, n: rt.at[:, lanes(o, n)], xp_s, xp_r)
    r_pair = pair(lambda o, n: r_out.at[srows(o, n), :], rp_s, rp_r)

    def all_of(copy, n):
        return [copy(p, i) for p in PIECES for i in range(n)]

    def start_own(ag, p):
        for n in range(4):
            ag(p, n).start()

    def pass_on(ag, p):
        for n in range(2):
            ag(p, n).wait_recv()
            ag(p, n + 4).start()

    def ring_and_pair(ag, pr):
        for p in PIECES:
            pass_on(ag, p)
            ag(p, 2).wait_recv()
            pr(p, 1).start()
            ag(p, 3).wait_recv()
            pr(p, 2).start()
        for p in PIECES:
            for n in range(2):
                ag(p, n + 4).wait_recv()
                pr(p, n + 3).start()
        for c in all_of(pr, 5):
            c.wait_recv()

    def combine():
        for p in PIECES:
            for n, j in ((0, 1), (1, 2)):
                x_rs(p, n).wait_recv()
                sl = rpos(p, n)
                pb[j, sl] = pb[j, sl] + xb[6 * p + n]
                x_rs(p, n + 4).start()

    def send_sums(j):
        for p in PIECES:
            for n in ((0, 1), (2,), (3,), ())[j]:
                x_rs(p, n).start()

    def scatter_first():
        def step(i, c):
            j, who = i // 2, i % 2
            ub[i] = first_product(i).astype(BF16)

            @pl.when(who == 0)
            def _():
                sib_copy(j).start()

            @pl.when(who == 1)
            def _():
                sib_copy(j).wait_recv()
                pb[j] = ub[i].astype(F32) + sb[j].astype(F32)
            for jj in range(3):
                @pl.when(i == 2 * jj + 1)
                def _():
                    send_sums(jj)

            @pl.when(i == 5)
            def _():
                combine()
            return c
        lax.fori_loop(0, nf, step, 0)

    def scatter_last():
        for i in (0, 2, 4, 1, 6, 3, 5, 7):
            j, who = i // 2, i % 2
            u = last_product(i).astype(BF16)
            if who == 0:
                ub[i] = u
                sib_copy(j).start()
            else:
                sib_copy(j).wait_recv()
                pb[j] = u.astype(F32) + sb[j].astype(F32)
                send_sums(j)
        combine()

    def finish_piece(p, scale):
        for h, a, b in ((0, 3, 4), (1, 2, 5)):
            x_rs(p, a).wait_recv()
            x_rs(p, b).wait_recv()
            sl = rpos(p, h)
            res[sl] = res[sl] - scale * (pb[3, sl] + xb[6 * p + a] + xb[6 * p + b])

    def first_product(i):
        xload(i).wait()

        @pl.when(i + 3 < nf)
        def _():
            xload(i + 3).start()
        return jnp.dot(x[srows(row_chunk(i) * rc, rc), :], w0b[...], preferred_element_type=F32)

    def part(d, p, first):
        nb = 2
        step = rows // nb

        def body(i, c):
            rs = srows(i * step, step)
            cs = lanes(d * fc + p * fh, fh)
            v = lax.dot_general(x[rs, cs], st[:, cs], NT, preferred_element_type=F32)
            ua[rs, :] = v if first else ua[rs, :] + v
            return c
        lax.fori_loop(0, nb, body, 0)

    def last_product(i):
        rs = srows(row_chunk(i) * rc, rc)
        cs = lanes(y_op * fc, fc)
        return ua[rs, :] + lax.dot_general(x[rs, cs], st[:, cs], NT, preferred_element_type=F32)

    def sweep(k, carry):
        scale = jnp.where(k == 0, 1.0, STEP_WEIGHT).astype(F32)
        for p in PIECES:
            finish_piece(p, scale)
            rt[:, lanes(fi * rc + p * rh, rh)] = jnp.transpose(res[pl.ds(p * rh, rh)]).astype(BF16)
            start_own(x_ag, p)
            x_pair(p, 0).start()
        wait_sends([sib_copy(j) for j in range(nx)])
        wait_sends(all_of(x_rs, 6))
        ring_and_pair(x_ag, x_pair)

        def g_step(i, c):
            j, q = i // 2, i % 2
            col = lanes(((yi + ring_off(j)) % ny) * fc + q * fh, fh)
            gp[:, col] = jnp.dot(rt[...], x[:, col], preferred_element_type=F32)
            for p in PIECES:
                for jj, ns in ((0, (0, 1)), (1, (2,)), (2, (3,))):
                    @pl.when(i == 2 * jj + p)
                    def _():
                        for n in ns:
                            y_rs(p, n).start()
            return c
        lax.fori_loop(0, 2 * ny, g_step, 0)
        wait_sends(all_of(x_ag, 6) + all_of(x_pair, 5))
        for p in PIECES:
            for n, d in ((0, y_up), (1, y_dn)):
                y_rs(p, n).wait_recv()
                col = gpos(d, p, n)
                gp[:, col] = gp[:, col] + yb[6 * p + n]
                y_rs(p, n + 4).start()

        for p in PIECES:
            for h, a, b in ((0, 3, 4), (1, 2, 5)):
                y_rs(p, a).wait_recv()
                y_rs(p, b).wait_recv()
                own = gpos(yi, p, h)
                wsl = pl.ds(p * fh + h * fq, fq)
                g = (gp[:, own] + yb[6 * p + a] + yb[6 * p + b]) * inv_total
                w = wt[:, wsl]
                s = eta_ref[:, own] * (g - lam_col[...] * w)
                wt[:, wsl] = w + STEP_WEIGHT * s
                st[:, own] = s.astype(BF16)
            start_own(y_ag, p)
            part(yi, p, p == 0)
        pass_on(y_ag, 0)
        for n in (2, 3):
            y_ag(0, n).wait_recv()
        part(y_dn, 0, False)
        pass_on(y_ag, 1)
        part(y_up, 0, False)
        for n in (2, 3):
            y_ag(1, n).wait_recv()
        part(y_dn, 1, False)
        part(y_up, 1, False)
        wait_sends(all_of(y_rs, 6))

        @pl.when(k == SWEEPS - 1)
        def _():
            w_out[srows(yi * fc, fc), :] = jnp.transpose(wt[...])
        for p in PIECES:
            for n in (4, 5):
                y_ag(p, n).wait_recv()

        @pl.when(k == SWEEPS - 1)
        def _():
            for p in PIECES:
                start_own(w_ag, p)
        scatter_last()
        wait_sends(all_of(y_ag, 6))
        return carry

    scatter_first()
    lax.fori_loop(0, SWEEPS, sweep, 0)

    for p in PIECES:
        finish_piece(p, STEP_WEIGHT)
        r_out[srows(fi * rc + p * rh, rh), :] = res[pl.ds(p * rh, rh)]
        start_own(r_ag, p)
        r_pair(p, 0).start()
    for p in PIECES:
        pass_on(w_ag, p)
    wait_sends([sib_copy(j) for j in range(nx)])
    wait_sends(all_of(x_rs, 6))

    ring_and_pair(r_ag, r_pair)
    for p in PIECES:
        for n in range(2, 6):
            w_ag(p, n).wait_recv()
    wait_sends(all_of(w_ag, 6) + all_of(r_ag, 6) + all_of(r_pair, 5))


def solution(mesh):
    ny, nf = mesh.shape["samp"], mesh.shape["feat"]
    design_spec = P(("problem", "samp"), "feat")
    rows_spec = P(("problem", "samp"), None)
    coef_spec = P(("problem", "feat"), None)
    step_spec = P(("problem", "feat"))
    ridge_spec = P("problem")

    def local_sweeps(design, targets, coef_init, step_sizes, ridge_weights):
        rows, feats = design.shape
        nt = targets.shape[1]
        rc, fc = rows // nf, feats // ny
        nx = nf // CORES
        dma = lambda n: pltpu.SemaphoreType.DMA((n,))
        anyspec = pl.BlockSpec(memory_space=pl.ANY)
        vspec = pl.BlockSpec(memory_space=pltpu.VMEM)
        return pl.pallas_call(
            functools.partial(sweeps_kernel, ny, nf),
            out_shape=(pltpu.VMEM((feats, nt), F32), pltpu.VMEM((rows, nt), F32)),
            in_specs=[anyspec, anyspec, anyspec, vspec, vspec],
            out_specs=(vspec, vspec),
            scratch_shapes=[
                pltpu.VMEM((rows, feats), BF16),
                pltpu.VMEM((nt, feats), BF16),
                pltpu.VMEM((nt, rows), BF16),
                pltpu.VMEM((nt, feats), F32),
                pltpu.VMEM((12, nt, fc // 4), F32),
                pltpu.VMEM((nf, rc, nt), BF16),
                pltpu.VMEM((nx, rc, nt), BF16),
                pltpu.VMEM((nx, rc, nt), F32),
                pltpu.VMEM((12, rc // 4, nt), F32),
                pltpu.VMEM((nt, fc), F32),
                pltpu.VMEM((rc, nt), F32),
                pltpu.VMEM((rows, nt), F32),
                pltpu.VMEM((feats, nt), BF16),
                pltpu.VMEM((nt, fc // 4), F32),
                dma(nf), dma(2), dma(nx), dma(nx), dma(12), dma(12), dma(12), dma(12),
                dma(12), dma(12), dma(10), dma(10), dma(12), dma(12), dma(12), dma(12), dma(12), dma(12), dma(10), dma(10),
            ],
            compiler_params=pltpu.CompilerParams(
                collective_id=0, has_side_effects=True, vmem_limit_bytes=54 * 1024 * 1024),
            name="sweeps",
        )(design, targets, coef_init, step_sizes[None, :], ridge_weights[None, :])
    return jax.shard_map(local_sweeps, mesh=mesh, in_specs=(design_spec, rows_spec, coef_spec, step_spec, ridge_spec),
                         out_specs=(coef_spec, rows_spec), check_vma=False)
```

```python
import functools

import jax
import jax.numpy as jnp
from jax import lax
from jax.experimental import pallas as pl
from jax.experimental.pallas import tpu as pltpu
from jax.sharding import PartitionSpec as P

SWEEPS = 4
STEP_WEIGHT = 0.5
CORES = 2
NT = (((1,), (1,)), ((), ()))
MESH = pl.DeviceIdType.MESH
BF16 = jnp.bfloat16
F32 = jnp.float32


def sweeps_kernel(ny, nf, x_hbm, y_hbm, w0_hbm, eta_ref, lam_ref, w_out, r_out,
                  x, st, rt, gp, yb, ub, sb, pb, xb, wt, res, ua, w0b, lam_col,
                  xsem, lsem, sib_s, sib_r, xs_s, xs_r, ys_s, ys_r,
                  xg_s, xg_r, xp_s, xp_r, yg_s, yg_r, wg_s, wg_r, rg_s, rg_r, rp_s, rp_r):
    nx = nf // CORES
    rows, feats = x.shape
    targets = wt.shape[0]
    rc = rows // nf
    rh = rc // 2
    fc = feats // ny
    fh = fc // 2
    inv_total = 1.0 / (rows * ny)

    yi = lax.axis_index("samp")
    fi = lax.axis_index("feat")
    chip = fi // CORES
    core = fi % CORES
    y_up, y_dn = (yi + 1) % ny, (yi + ny - 1) % ny
    y_op = (yi + 2) % ny
    c_up, c_dn = (chip + 1) % nx, (chip + nx - 1) % nx
    c_op = (chip + 2) % nx
    UP = {"feat": c_up * CORES + core}
    DN = {"feat": c_dn * CORES + core}
    SIB = {"feat": chip * CORES + 1 - core}
    UPX = {"feat": c_up * CORES + 1 - core}
    DNX = {"feat": c_dn * CORES + 1 - core}
    YUP = {"samp": y_up}
    YDN = {"samp": y_dn}

    def rcopy(src, dst, ss, rs, dev):
        return pltpu.make_async_remote_copy(src_ref=src, dst_ref=dst, send_sem=ss, recv_sem=rs,
                                            device_id=dev, device_id_type=MESH)

    def lanes(start, size):
        return pl.ds(pl.multiple_of(start, 128), size)

    def srows(start, size):
        return pl.ds(pl.multiple_of(start, 128), size)

    def erows(start, size):
        return pl.ds(pl.multiple_of(start, 8), size)

    def ring_off(j):
        return (2 + 3 * j + 3 * (j // 2) + 2 * (j // 3)) % 4

    def row_chunk(i):
        j, who = i // 2, i % 2
        d = (chip + ring_off(j)) % nx
        return d * CORES + core + (1 - who) * (1 - 2 * core)

    def xload(i):
        c = row_chunk(i)
        return pltpu.make_async_copy(x_hbm.at[srows(c * rc, rc), :], x.at[srows(c * rc, rc), :], xsem.at[i])

    w0_copy = pltpu.make_async_copy(w0_hbm, w_out, lsem.at[0])
    y_copy = pltpu.make_async_copy(y_hbm.at[srows(fi * rc, rc), :], res, lsem.at[1])
    w0_copy.start()
    for i in range(1):
        xload(i).start()
    y_copy.start()

    barrier = pltpu.get_barrier_semaphore()
    peers = (UP, DN, UPX, DNX, SIB, YUP, YDN)
    for dev in peers:
        pl.semaphore_signal(barrier, inc=1, device_id=dev, device_id_type=MESH)

    w0_copy.wait()
    for i in range(1, 3):
        xload(i).start()

    w0b[...] = w_out[...].astype(BF16)
    pl.semaphore_wait(barrier, len(peers))

    PIECES = range(2)
    FINE = range(4)
    rq, fq = rc // 4, fc // 4
    re = rc // 4

    def wait_sends(copies):
        for c in copies:
            c().wait_send()

    def wait_recvs(copies):
        for c in copies:
            c().wait_recv()

    def sib_copy(j):
        return rcopy(ub.at[2 * j], sb.at[j], sib_s.at[j], sib_r.at[j], SIB)

    def rpos(p, h):
        return pl.ds(p * rh + h * rq, rq)

    def x_rs(p, n):
        j, h = ((0, 0), (0, 1), (1, 1), (2, 0), (1, 0), (2, 1))[n]
        return rcopy(pb.at[j, rpos(p, h)], xb.at[6 * p + n], xs_s.at[6 * p + n], xs_r.at[6 * p + n], (UP, DN)[n % 2])

    def gpos(d, p, h):
        return lanes(d * fc + p * 2 * fq + h * fq, fq)

    def y_rs(p, n):
        d, h = ((y_op, 0), (y_op, 1), (y_up, 1), (y_dn, 0), (y_up, 0), (y_dn, 1))[n]
        return rcopy(gp.at[:, gpos(d, p, h)], yb.at[6 * p + n], ys_s.at[6 * p + n], ys_r.at[6 * p + n], (YUP, YDN)[n % 2])

    def ring(at, ss, rs, up, dn, me, below, above):
        def copy(p, n):
            d, h = ((me, 0), (me, 1), (me, 1), (me, 0), (below, 0), (above, 1))[n]
            src = at(d, p, h)
            return rcopy(src, src, ss.at[6 * p + n], rs.at[6 * p + n], (up, dn)[n % 2])
        return copy

    def cross(n):
        src = rt.at[:, lanes(xpos((c_dn, c_up)[n], 1, n), rq)]
        return rcopy(src, src, xp_s.at[8 + n], xp_r.at[8 + n], (UPX, DNX)[n])

    def xpos(d, p, h, size=rq):
        return (d * CORES + core) * rc + (2 * p + h) * size

    def wpos(d, p, h):
        return srows(d * fc + p * fh + h * fh // 2, fh // 2)

    y_ag = ring(lambda d, p, h: st.at[:, gpos(d, p, h)], yg_s, yg_r, YUP, YDN, yi, y_dn, y_up)
    x_ag = ring(lambda d, p, h: rt.at[:, lanes(xpos(d, p, h), rq)], xg_s, xg_r, UP, DN, chip, c_dn, c_up)
    w_ag = ring(lambda d, p, h: w_out.at[wpos(d, p, h), :], wg_s, wg_r, YUP, YDN, yi, y_dn, y_up)
    r_ag = ring(lambda d, p, h: r_out.at[erows(xpos(d, p, h, re), re), :], rg_s, rg_r, UP, DN, chip, c_dn, c_up)

    def pair(at, unit, ss, rs):
        def copy(p, n):
            d, h, units = ((chip, 0, 2), (c_dn, 0, 2), (c_up, 0, 2), (c_op, 0, 1), (c_op, 1, 1))[n]
            src = at(xpos(d, p, h, unit), units * unit)
            return rcopy(src, src, ss.at[5 * p + n], rs.at[5 * p + n], SIB)
        return copy

    x_pair = pair(lambda o, n: rt.at[:, lanes(o, n)], rq, xp_s, xp_r)
    r_pair = pair(lambda o, n: r_out.at[erows(o, n), :], re, rp_s, rp_r)

    def all_of(copy, n, pieces=PIECES):
        return [functools.partial(copy, p, i) for p in pieces for i in range(n)]

    def start_own(ag, p):
        for n in range(4):
            ag(p, n).start()

    def pass_on(ag, p):
        for n in range(2):
            ag(p, n).wait_recv()
            ag(p, n + 4).start()

    def near(pr, p):
        return [functools.partial(pr, p, n) for n in range(3)]

    def far(pr, p):
        return [functools.partial(pr, p, n) for n in (3, 4)]

    crosses = [functools.partial(cross, 0), functools.partial(cross, 1)]

    def ring_and_pair(ag, pr, pieces, crossed, meanwhile):
        last = len(pieces) - 1
        for p in pieces:
            for n in range(2):
                ag(p, n).wait_recv()
                ag(p, n + 4).start()
                if crossed and p == last:
                    cross(n).start()
            ag(p, 2).wait_recv()
            pr(p, 1).start()
            ag(p, 3).wait_recv()
            pr(p, 2).start()
        for p in pieces:
            if p == last:
                wait_recvs([c for q in pieces for c in near(pr, q)])
                if meanwhile is not None:
                    meanwhile()
            for n in range(2):
                ag(p, n + 4).wait_recv()
                if not (crossed and p == last):
                    pr(p, n + 3).start()
        for p in pieces:
            wait_recvs(crosses if crossed and p == last else far(pr, p))

    def combine():
        for p in PIECES:
            for n, j in ((0, 1), (1, 2)):
                x_rs(p, n).wait_recv()
                sl = rpos(p, n)
                pb[j, sl] = pb[j, sl] + xb[6 * p + n]
                x_rs(p, n + 4).start()

    def send_sums(j):
        for p in PIECES:
            for n in ((0, 1), (2,), (3,), ())[j]:
                x_rs(p, n).start()

    def scatter_first():
        def step(i, c):
            j, who = i // 2, i % 2
            ub[i] = first_product(i).astype(BF16)

            @pl.when(who == 0)
            def _():
                sib_copy(j).start()

            @pl.when(who == 1)
            def _():
                sib_copy(j).wait_recv()
                pb[j] = ub[i].astype(F32) + sb[j].astype(F32)
            for jj in range(3):
                @pl.when(i == 2 * jj + 1)
                def _():
                    send_sums(jj)

            @pl.when(i == 5)
            def _():
                combine()
            return c
        lax.fori_loop(0, nf, step, 0)

    def scatter_last():
        def make(i):
            ub[i] = last_product(i).astype(BF16)
            if i % 2 == 0:
                sib_copy(i // 2).start()

        def close(j):
            sib_copy(j).wait_recv()
            pb[j] = ub[2 * j + 1].astype(F32) + sb[j].astype(F32)
            send_sums(j)

        for i in (0, 1, 2):
            make(i)
        close(0)
        make(4)
        make(3)
        close(1)
        make(5)
        close(2)
        make(6)
        make(7)
        close(3)
        combine()

    def finish_piece(p, scale):
        for h, a, b in ((0, 3, 4), (1, 2, 5)):
            x_rs(p, a).wait_recv()
            x_rs(p, b).wait_recv()
            sl = rpos(p, h)
            res[sl] = res[sl] - scale * (pb[3, sl] + xb[6 * p + a] + xb[6 * p + b])

    def first_product(i):
        xload(i).wait()

        @pl.when(i + 3 < nf)
        def _():
            xload(i + 3).start()
        return jnp.dot(x[srows(row_chunk(i) * rc, rc), :], w0b[...], preferred_element_type=F32)

    def part(d, p, first):
        nb = 2
        step = rows // nb

        def body(i, c):
            rs = srows(i * step, step)
            cs = lanes(d * fc + p * fh, fh)
            v = lax.dot_general(x[rs, cs], st[:, cs], NT, preferred_element_type=F32)
            ua[rs, :] = v if first else ua[rs, :] + v
            return c
        lax.fori_loop(0, nb, body, 0)

    def last_product(i):
        rs = srows(row_chunk(i) * rc, rc)
        cs = lanes(y_op * fc, fc)
        return ua[rs, :] + lax.dot_general(x[rs, cs], st[:, cs], NT, preferred_element_type=F32)

    def sweep(k, carry):
        scale = jnp.where(k == 0, 1.0, STEP_WEIGHT).astype(F32)
        for p in PIECES:
            finish_piece(p, scale)
            rt[:, lanes(fi * rc + p * rh, rh)] = jnp.transpose(res[pl.ds(p * rh, rh)]).astype(BF16)
            start_own(x_ag, p)
            x_pair(p, 0).start()
        wait_sends([functools.partial(sib_copy, j) for j in range(nx)])
        wait_sends(all_of(x_rs, 6))
        rows_of = CORES * rc

        def chip_dot(d, col):
            return jnp.dot(rt[:, lanes(d * rows_of, rows_of)], x[srows(d * rows_of, rows_of), col],
                           preferred_element_type=F32)

        def g_early():
            for q in PIECES:
                col = lanes(y_op * fc + q * fh, fh)
                gp[:, col] = chip_dot(chip, col) + chip_dot(c_up, col) + chip_dot(c_dn, col)
        ring_and_pair(x_ag, x_pair, PIECES, True, g_early)

        for p in PIECES:
            col = lanes(y_op * fc + p * fh, fh)
            gp[:, col] = gp[:, col] + chip_dot(c_op, col)
            y_rs(p, 0).start()
            y_rs(p, 1).start()

        def g_step(i, c):
            j, q = i // 2, i % 2
            col = lanes(((yi + ring_off(j)) % ny) * fc + q * fh, fh)
            gp[:, col] = jnp.dot(rt[...], x[:, col], preferred_element_type=F32)
            for p in PIECES:
                for jj in (1, 2):
                    @pl.when(i == 2 * jj + p)
                    def _():
                        y_rs(p, jj + 1).start()
            return c
        lax.fori_loop(2, 2 * ny, g_step, 0)
        wait_sends(all_of(x_ag, 6) + near(x_pair, 0) + near(x_pair, 1) + far(x_pair, 0) + crosses)
        for p in PIECES:
            for n, d in ((0, y_up), (1, y_dn)):
                y_rs(p, n).wait_recv()
                col = gpos(d, p, n)
                gp[:, col] = gp[:, col] + yb[6 * p + n]
                y_rs(p, n + 4).start()

        for p in PIECES:
            for h, a, b in ((0, 3, 4), (1, 2, 5)):
                y_rs(p, a).wait_recv()
                y_rs(p, b).wait_recv()
                own = gpos(yi, p, h)
                wsl = pl.ds((2 * p + h) * fq, fq)
                g = (gp[:, own] + yb[6 * p + a] + yb[6 * p + b]) * inv_total
                w = wt[:, wsl]
                s = eta_ref[:, own] * (g - lam_col[...] * w)
                wt[:, wsl] = w + STEP_WEIGHT * s
                st[:, own] = s.astype(BF16)
            start_own(y_ag, p)
            part(yi, p, p == 0)

        def own_in(p):
            for n in (2, 3):
                y_ag(p, n).wait_recv()

        pass_on(y_ag, 0)
        own_in(0)
        part(y_dn, 0, False)
        pass_on(y_ag, 1)

        @pl.when(k == SWEEPS - 1)
        def _():
            w_out[srows(yi * fc, fc), :] = jnp.transpose(wt[...])
            for p in PIECES:
                start_own(w_ag, p)
        part(y_up, 0, False)
        own_in(1)
        part(y_dn, 1, False)
        part(y_up, 1, False)
        wait_sends(all_of(y_rs, 6))

        for p in PIECES:
            for n in (4, 5):
                y_ag(p, n).wait_recv()

        scatter_last()
        wait_sends(all_of(y_ag, 6))
        return carry

    scatter_first()
    lam_col[...] = jnp.transpose(jnp.broadcast_to(lam_ref[...], (lam_col.shape[1], targets)))
    for h in range(2):
        wt[:, pl.ds(h * fh, fh)] = jnp.transpose(w_out[srows(yi * fc + h * fh, fh), :])
    y_copy.wait()
    lax.fori_loop(0, SWEEPS, sweep, 0)

    for p in PIECES:
        pass_on(w_ag, p)
    for p in PIECES:
        finish_piece(p, STEP_WEIGHT)
        r_out[srows(fi * rc + p * rh, rh), :] = res[pl.ds(p * rh, rh)]
        start_own(r_ag, p)
        r_pair(p, 0).start()
    wait_sends([functools.partial(sib_copy, j) for j in range(nx)])
    wait_sends(all_of(x_rs, 6))

    ring_and_pair(r_ag, r_pair, PIECES, False, None)
    for p in PIECES:
        for n in range(2, 6):
            w_ag(p, n).wait_recv()
    wait_sends(all_of(w_ag, 6) + all_of(r_ag, 6) + all_of(r_pair, 5))


def solution(mesh):
    ny, nf = mesh.shape["samp"], mesh.shape["feat"]
    design_spec = P(("problem", "samp"), "feat")
    rows_spec = P(("problem", "samp"), None)
    coef_spec = P(("problem", "feat"), None)
    step_spec = P(("problem", "feat"))
    ridge_spec = P("problem")

    def local_sweeps(design, targets, coef_init, step_sizes, ridge_weights):
        rows, feats = design.shape
        nt = targets.shape[1]
        rc, fc = rows // nf, feats // ny
        nx = nf // CORES
        dma = lambda n: pltpu.SemaphoreType.DMA((n,))
        anyspec = pl.BlockSpec(memory_space=pl.ANY)
        vspec = pl.BlockSpec(memory_space=pltpu.VMEM)
        return pl.pallas_call(
            functools.partial(sweeps_kernel, ny, nf),
            out_shape=(pltpu.VMEM((feats, nt), F32), pltpu.VMEM((rows, nt), F32)),
            in_specs=[anyspec, anyspec, anyspec, vspec, vspec],
            out_specs=(vspec, vspec),
            scratch_shapes=[
                pltpu.VMEM((rows, feats), BF16),
                pltpu.VMEM((nt, feats), BF16),
                pltpu.VMEM((nt, rows), BF16),
                pltpu.VMEM((nt, feats), F32),
                pltpu.VMEM((12, nt, fc // 4), F32),
                pltpu.VMEM((nf, rc, nt), BF16),
                pltpu.VMEM((nx, rc, nt), BF16),
                pltpu.VMEM((nx, rc, nt), F32),
                pltpu.VMEM((12, rc // 4, nt), F32),
                pltpu.VMEM((nt, fc), F32),
                pltpu.VMEM((rc, nt), F32),
                pltpu.VMEM((rows, nt), F32),
                pltpu.VMEM((feats, nt), BF16),
                pltpu.VMEM((nt, fc // 4), F32),
                dma(nf), dma(2), dma(nx), dma(nx), dma(12), dma(12), dma(12), dma(12),
                dma(12), dma(12), dma(10), dma(10), dma(12), dma(12), dma(12), dma(12), dma(24), dma(24), dma(20), dma(20),
            ],
            compiler_params=pltpu.CompilerParams(
                collective_id=0, has_side_effects=True, vmem_limit_bytes=54 * 1024 * 1024),
            name="sweeps",
        )(design, targets, coef_init, step_sizes[None, :], ridge_weights[None, :])
    return jax.shard_map(local_sweeps, mesh=mesh, in_specs=(design_spec, rows_spec, coef_spec, step_spec, ridge_spec),
                         out_specs=(coef_spec, rows_spec), check_vma=False)
```

```python
import functools

import jax
import jax.numpy as jnp
from jax import lax
from jax.experimental import pallas as pl
from jax.experimental.pallas import tpu as pltpu
from jax.sharding import PartitionSpec as P

SWEEPS = 4
STEP_WEIGHT = 0.5
CORES = 2
NT = (((1,), (1,)), ((), ()))
MESH = pl.DeviceIdType.MESH
BF16 = jnp.bfloat16
F32 = jnp.float32


def sweeps_kernel(ny, nf, x_hbm, y_hbm, w0_hbm, eta_ref, lam_ref, w_out, r_out,
                  x, st, rt, gp, yb, ub, sb, pb, xb, wt, res, ua, w0b, lam_col,
                  xsem, lsem, sib_s, sib_r, xs_s, xs_r, ys_s, ys_r,
                  xg_s, xg_r, xp_s, xp_r, yg_s, yg_r, wg_s, wg_r, rg_s, rg_r, rp_s, rp_r):
    nx = nf // CORES
    rows, feats = x.shape
    targets = wt.shape[0]
    rc = rows // nf
    rh = rc // 2
    fc = feats // ny
    fh = fc // 2
    inv_total = 1.0 / (rows * ny)

    yi = lax.axis_index("samp")
    fi = lax.axis_index("feat")
    chip = fi // CORES
    core = fi % CORES
    y_up, y_dn = (yi + 1) % ny, (yi + ny - 1) % ny
    y_op = (yi + 2) % ny
    c_up, c_dn = (chip + 1) % nx, (chip + nx - 1) % nx
    c_op = (chip + 2) % nx
    UP = {"feat": c_up * CORES + core}
    DN = {"feat": c_dn * CORES + core}
    SIB = {"feat": chip * CORES + 1 - core}
    UPX = {"feat": c_up * CORES + 1 - core}
    DNX = {"feat": c_dn * CORES + 1 - core}
    YUP = {"samp": y_up}
    YDN = {"samp": y_dn}

    def rcopy(src, dst, ss, rs, dev):
        return pltpu.make_async_remote_copy(src_ref=src, dst_ref=dst, send_sem=ss, recv_sem=rs,
                                            device_id=dev, device_id_type=MESH)

    def lanes(start, size):
        return pl.ds(pl.multiple_of(start, 128), size)

    def srows(start, size):
        return pl.ds(pl.multiple_of(start, 128), size)

    def ring_off(j):
        return (2 + 3 * j + 3 * (j // 2) + 2 * (j // 3)) % 4

    def row_chunk(i):
        j, who = i // 2, i % 2
        d = (chip + ring_off(j)) % nx
        return d * CORES + core + (1 - who) * (1 - 2 * core)

    def xload(i):
        c = row_chunk(i)
        return pltpu.make_async_copy(x_hbm.at[srows(c * rc, rc), :], x.at[srows(c * rc, rc), :], xsem.at[i])

    w0_copy = pltpu.make_async_copy(w0_hbm, w_out, lsem.at[0])
    y_copy = pltpu.make_async_copy(y_hbm.at[srows(fi * rc, rc), :], res, lsem.at[1])
    w0_copy.start()
    for i in range(1):
        xload(i).start()
    y_copy.start()

    barrier = pltpu.get_barrier_semaphore()
    peers = (UP, DN, UPX, DNX, SIB, YUP, YDN)
    for dev in peers:
        pl.semaphore_signal(barrier, inc=1, device_id=dev, device_id_type=MESH)

    w0_copy.wait()
    for i in range(1, 3):
        xload(i).start()

    w0b[...] = w_out[...].astype(BF16)
    lam_col[...] = jnp.transpose(jnp.broadcast_to(lam_ref[...], (lam_col.shape[1], targets)))
    for h in range(2):
        wt[:, pl.ds(h * fh, fh)] = jnp.transpose(w_out[srows(yi * fc + h * fh, fh), :])
    pl.semaphore_wait(barrier, len(peers))
    y_copy.wait()

    PIECES = range(2)
    rq, fq = rc // 4, fc // 4

    def wait_sends(copies):
        for c in copies:
            c.wait_send()

    def sib_copy(j):
        return rcopy(ub.at[2 * j], sb.at[j], sib_s.at[j], sib_r.at[j], SIB)

    def rpos(p, h):
        return pl.ds(p * rh + h * rq, rq)

    def x_rs(p, n):
        j, h = ((0, 0), (0, 1), (1, 1), (2, 0), (1, 0), (2, 1))[n]
        return rcopy(pb.at[j, rpos(p, h)], xb.at[6 * p + n], xs_s.at[6 * p + n], xs_r.at[6 * p + n], (UP, DN)[n % 2])

    def gpos(d, p, h):
        return lanes(d * fc + p * fh + h * fq, fq)

    def y_rs(p, n):
        d, h = ((y_op, 0), (y_op, 1), (y_up, 1), (y_dn, 0), (y_up, 0), (y_dn, 1))[n]
        return rcopy(gp.at[:, gpos(d, p, h)], yb.at[6 * p + n], ys_s.at[6 * p + n], ys_r.at[6 * p + n], (YUP, YDN)[n % 2])

    def ring(at, ss, rs, up, dn, me, below, above):
        def copy(p, n):
            d, h = ((me, 0), (me, 1), (me, 1), (me, 0), (below, 0), (above, 1))[n]
            src = at(d, p, h)
            return rcopy(src, src, ss.at[6 * p + n], rs.at[6 * p + n], (up, dn)[n % 2])
        return copy

    def cross(n):
        src = rt.at[:, lanes(xpos((c_dn, c_up)[n], 1, n), rq)]
        return rcopy(src, src, xp_s.at[8 + n], xp_r.at[8 + n], (UPX, DNX)[n])

    def xpos(d, p, h):
        return (d * CORES + core) * rc + p * rh + h * rq

    def wpos(d, p, h):
        return srows(d * fc + p * fh + h * fq, fq)

    y_ag = ring(lambda d, p, h: st.at[:, gpos(d, p, h)], yg_s, yg_r, YUP, YDN, yi, y_dn, y_up)
    x_ag = ring(lambda d, p, h: rt.at[:, lanes(xpos(d, p, h), rq)], xg_s, xg_r, UP, DN, chip, c_dn, c_up)
    w_ag = ring(lambda d, p, h: w_out.at[wpos(d, p, h), :], wg_s, wg_r, YUP, YDN, yi, y_dn, y_up)
    r_ag = ring(lambda d, p, h: r_out.at[srows(xpos(d, p, h), rq), :], rg_s, rg_r, UP, DN, chip, c_dn, c_up)

    def pair(at, ss, rs):
        def copy(p, n):
            d, h, size = ((chip, 0, rh), (c_dn, 0, rh), (c_up, 0, rh), (c_op, 0, rq), (c_op, 1, rq))[n]
            src = at(xpos(d, p, h), size)
            return rcopy(src, src, ss.at[5 * p + n], rs.at[5 * p + n], SIB)
        return copy

    x_pair = pair(lambda o, n: rt.at[:, lanes(o, n)], xp_s, xp_r)
    r_pair = pair(lambda o, n: r_out.at[srows(o, n), :], rp_s, rp_r)

    def all_of(copy, n):
        return [copy(p, i) for p in PIECES for i in range(n)]

    def pairs(pr, crossed):
        return [pr(0, n) for n in range(5)] + [pr(1, n) for n in range(3)] + (
            [cross(0), cross(1)] if crossed else [pr(1, 3), pr(1, 4)])

    def start_own(ag, p):
        for n in range(4):
            ag(p, n).start()

    def pass_on(ag, p):
        for n in range(2):
            ag(p, n).wait_recv()
            ag(p, n + 4).start()

    def ring_and_pair(ag, pr, crossed, meanwhile):
        for p in PIECES:
            for n in range(2):
                ag(p, n).wait_recv()
                ag(p, n + 4).start()
                if crossed and p == 1:
                    cross(n).start()
            ag(p, 2).wait_recv()
            pr(p, 1).start()
            ag(p, 3).wait_recv()
            pr(p, 2).start()
        for p in PIECES:
            if p == 1:
                for c in pairs(pr, crossed)[:3] + pairs(pr, crossed)[5:8]:
                    c.wait_recv()
                if meanwhile is not None:
                    meanwhile()
            for n in range(2):
                ag(p, n + 4).wait_recv()
                if not (crossed and p == 1):
                    pr(p, n + 3).start()
        for c in pairs(pr, crossed)[3:5] + pairs(pr, crossed)[8:]:
            c.wait_recv()

    def combine():
        for p in PIECES:
            for n, j in ((0, 1), (1, 2)):
                x_rs(p, n).wait_recv()
                sl = rpos(p, n)
                pb[j, sl] = pb[j, sl] + xb[6 * p + n]
                x_rs(p, n + 4).start()

    def send_sums(j):
        for p in PIECES:
            for n in ((0, 1), (2,), (3,), ())[j]:
                x_rs(p, n).start()

    def scatter_first():
        def step(i, c):
            j, who = i // 2, i % 2
            ub[i] = first_product(i).astype(BF16)

            @pl.when(who == 0)
            def _():
                sib_copy(j).start()

            @pl.when(who == 1)
            def _():
                sib_copy(j).wait_recv()
                pb[j] = ub[i].astype(F32) + sb[j].astype(F32)
            for jj in range(3):
                @pl.when(i == 2 * jj + 1)
                def _():
                    send_sums(jj)

            @pl.when(i == 5)
            def _():
                combine()
            return c
        lax.fori_loop(0, nf, step, 0)

    def scatter_last():
        def make(i):
            ub[i] = last_product(i).astype(BF16)
            if i % 2 == 0:
                sib_copy(i // 2).start()

        def close(j):
            sib_copy(j).wait_recv()
            pb[j] = ub[2 * j + 1].astype(F32) + sb[j].astype(F32)
            send_sums(j)

        for i in (0, 1, 2):
            make(i)
        close(0)
        make(4)
        make(3)
        close(1)
        make(5)
        close(2)
        make(6)
        make(7)
        close(3)
        combine()

    def finish_piece(p, scale):
        for h, a, b in ((0, 3, 4), (1, 2, 5)):
            x_rs(p, a).wait_recv()
            x_rs(p, b).wait_recv()
            sl = rpos(p, h)
            res[sl] = res[sl] - scale * (pb[3, sl] + xb[6 * p + a] + xb[6 * p + b])

    def first_product(i):
        xload(i).wait()

        @pl.when(i + 3 < nf)
        def _():
            xload(i + 3).start()
        return jnp.dot(x[srows(row_chunk(i) * rc, rc), :], w0b[...], preferred_element_type=F32)

    def part(d, p, first):
        nb = 2
        step = rows // nb

        def body(i, c):
            rs = srows(i * step, step)
            cs = lanes(d * fc + p * fh, fh)
            v = lax.dot_general(x[rs, cs], st[:, cs], NT, preferred_element_type=F32)
            ua[rs, :] = v if first else ua[rs, :] + v
            return c
        lax.fori_loop(0, nb, body, 0)

    def last_product(i):
        rs = srows(row_chunk(i) * rc, rc)
        cs = lanes(y_op * fc, fc)
        return ua[rs, :] + lax.dot_general(x[rs, cs], st[:, cs], NT, preferred_element_type=F32)

    def sweep(k, carry):
        scale = jnp.where(k == 0, 1.0, STEP_WEIGHT).astype(F32)
        for p in PIECES:
            finish_piece(p, scale)
            rt[:, lanes(fi * rc + p * rh, rh)] = jnp.transpose(res[pl.ds(p * rh, rh)]).astype(BF16)
            start_own(x_ag, p)
            x_pair(p, 0).start()
        wait_sends([sib_copy(j) for j in range(nx)])
        wait_sends(all_of(x_rs, 6))
        rows_of = CORES * rc

        def chip_dot(d, col):
            return jnp.dot(rt[:, lanes(d * rows_of, rows_of)], x[srows(d * rows_of, rows_of), col],
                           preferred_element_type=F32)

        def g_early():
            for q in PIECES:
                col = lanes(y_op * fc + q * fh, fh)
                gp[:, col] = chip_dot(chip, col) + chip_dot(c_up, col) + chip_dot(c_dn, col)
        ring_and_pair(x_ag, x_pair, True, g_early)

        for p in PIECES:
            col = lanes(y_op * fc + p * fh, fh)
            gp[:, col] = gp[:, col] + chip_dot(c_op, col)
            y_rs(p, 0).start()
            y_rs(p, 1).start()

        def g_step(i, c):
            j, q = i // 2, i % 2
            col = lanes(((yi + ring_off(j)) % ny) * fc + q * fh, fh)
            gp[:, col] = jnp.dot(rt[...], x[:, col], preferred_element_type=F32)
            for p in PIECES:
                for jj in (1, 2):
                    @pl.when(i == 2 * jj + p)
                    def _():
                        y_rs(p, jj + 1).start()
            return c
        lax.fori_loop(2, 2 * ny, g_step, 0)
        wait_sends(all_of(x_ag, 6) + pairs(x_pair, True))
        for p in PIECES:
            for n, d in ((0, y_up), (1, y_dn)):
                y_rs(p, n).wait_recv()
                col = gpos(d, p, n)
                gp[:, col] = gp[:, col] + yb[6 * p + n]
                y_rs(p, n + 4).start()

        for p in PIECES:
            for h, a, b in ((0, 3, 4), (1, 2, 5)):
                y_rs(p, a).wait_recv()
                y_rs(p, b).wait_recv()
                own = gpos(yi, p, h)
                wsl = pl.ds(p * fh + h * fq, fq)
                g = (gp[:, own] + yb[6 * p + a] + yb[6 * p + b]) * inv_total
                w = wt[:, wsl]
                s = eta_ref[:, own] * (g - lam_col[...] * w)
                wt[:, wsl] = w + STEP_WEIGHT * s
                st[:, own] = s.astype(BF16)
            start_own(y_ag, p)
            part(yi, p, p == 0)
        pass_on(y_ag, 0)
        for n in (2, 3):
            y_ag(0, n).wait_recv()
        part(y_dn, 0, False)
        pass_on(y_ag, 1)
        part(y_up, 0, False)
        for n in (2, 3):
            y_ag(1, n).wait_recv()
        part(y_dn, 1, False)
        part(y_up, 1, False)
        wait_sends(all_of(y_rs, 6))

        @pl.when(k == SWEEPS - 1)
        def _():
            w_out[srows(yi * fc, fc), :] = jnp.transpose(wt[...])
        for p in PIECES:
            for n in (4, 5):
                y_ag(p, n).wait_recv()

        @pl.when(k == SWEEPS - 1)
        def _():
            for p in PIECES:
                start_own(w_ag, p)
        scatter_last()
        wait_sends(all_of(y_ag, 6))
        return carry

    scatter_first()
    lax.fori_loop(0, SWEEPS, sweep, 0)

    for p in PIECES:
        finish_piece(p, STEP_WEIGHT)
        r_out[srows(fi * rc + p * rh, rh), :] = res[pl.ds(p * rh, rh)]
        start_own(r_ag, p)
        r_pair(p, 0).start()
    for p in PIECES:
        pass_on(w_ag, p)
    wait_sends([sib_copy(j) for j in range(nx)])
    wait_sends(all_of(x_rs, 6))

    ring_and_pair(r_ag, r_pair, False, None)
    for p in PIECES:
        for n in range(2, 6):
            w_ag(p, n).wait_recv()
    wait_sends(all_of(w_ag, 6) + all_of(r_ag, 6) + all_of(r_pair, 5))


def solution(mesh):
    ny, nf = mesh.shape["samp"], mesh.shape["feat"]
    design_spec = P(("problem", "samp"), "feat")
    rows_spec = P(("problem", "samp"), None)
    coef_spec = P(("problem", "feat"), None)
    step_spec = P(("problem", "feat"))
    ridge_spec = P("problem")

    def local_sweeps(design, targets, coef_init, step_sizes, ridge_weights):
        rows, feats = design.shape
        nt = targets.shape[1]
        rc, fc = rows // nf, feats // ny
        nx = nf // CORES
        dma = lambda n: pltpu.SemaphoreType.DMA((n,))
        anyspec = pl.BlockSpec(memory_space=pl.ANY)
        vspec = pl.BlockSpec(memory_space=pltpu.VMEM)
        return pl.pallas_call(
            functools.partial(sweeps_kernel, ny, nf),
            out_shape=(pltpu.VMEM((feats, nt), F32), pltpu.VMEM((rows, nt), F32)),
            in_specs=[anyspec, anyspec, anyspec, vspec, vspec],
            out_specs=(vspec, vspec),
            scratch_shapes=[
                pltpu.VMEM((rows, feats), BF16),
                pltpu.VMEM((nt, feats), BF16),
                pltpu.VMEM((nt, rows), BF16),
                pltpu.VMEM((nt, feats), F32),
                pltpu.VMEM((12, nt, fc // 4), F32),
                pltpu.VMEM((nf, rc, nt), BF16),
                pltpu.VMEM((nx, rc, nt), BF16),
                pltpu.VMEM((nx, rc, nt), F32),
                pltpu.VMEM((12, rc // 4, nt), F32),
                pltpu.VMEM((nt, fc), F32),
                pltpu.VMEM((rc, nt), F32),
                pltpu.VMEM((rows, nt), F32),
                pltpu.VMEM((feats, nt), BF16),
                pltpu.VMEM((nt, fc // 4), F32),
                dma(nf), dma(2), dma(nx), dma(nx), dma(12), dma(12), dma(12), dma(12),
                dma(12), dma(12), dma(10), dma(10), dma(12), dma(12), dma(12), dma(12), dma(12), dma(12), dma(10), dma(10),
            ],
            compiler_params=pltpu.CompilerParams(
                collective_id=0, has_side_effects=True, vmem_limit_bytes=54 * 1024 * 1024),
            name="sweeps",
        )(design, targets, coef_init, step_sizes[None, :], ridge_weights[None, :])
    return jax.shard_map(local_sweeps, mesh=mesh, in_specs=(design_spec, rows_spec, coef_spec, step_spec, ridge_spec),
                         out_specs=(coef_spec, rows_spec), check_vma=False)
```
